32 devices in a mesh: fourier: 2 (over x), ex: 4 (over z), ey: 4 (over y, core).
Axes of the slice: x: 2, y: 2, z: 4, core: 2. Of those that a mesh axis runs over, the one named last changes fastest.
Arguments:
- forcing: float32 [128, 81, 2048], P('fourier', None, ('ex', 'ey')), may hold values from -6 to 6
- element_coef: float32 [2048], P(('ex', 'ey')), may hold values from 0.5 to 2
- schur: float32 [128, 32, 32], P('fourier'), may hold values from -12 to 20, as said below
- couple: float32 [128, 32, 49], P('fourier'), may hold values from -0.875 to 0.875
- inner_inv: float32 [128, 49, 49], P('fourier'), may hold values from -3 to 4.5, as said below
- element_cell: int32 [2048], P(('ex', 'ey')), may hold values from 0 to 127, as said below
Outputs:
- velocity: float32 [128, 81, 2048], P('fourier', None, ('ex', 'ey'))
The draws below stay inside these ranges and needn't reach their ends.
Inputs may be any that keep to these rules, and one draw needn't show every extreme that they name: `element_cell`: each aligned block of 128 entries is a permutation of 0 to 127. `schur`: each matrix is symmetric positive definite. `inner_inv`: each matrix is symmetric positive definite.
All inputs are finite; a program needn't handle non-finite values.
Results may differ from the reference program's by a relative error of at most 0.0001.
Values sent between devices are 32-bit elements; how exact they have to be, the bound alone decides.
A program may use at most 128 MiB of HBM per device.

```python
import math
import jax
import jax.numpy as jnp
import numpy as np
from jax import lax

P_SIZE = 8
NZ = 128
ITERS = 3
ELX = 8
ELY = 16
NODES = 81
NB = 32
NI = 49
EL_DEV = 128
ELEMENTS = 2048
NXE = 32
NYE = 64
N_EY = 4


def draw_schur(key, part):
    first, second = jax.random.split(jax.random.fold_in(key, 11), 2)
    width = 4 * P_SIZE
    factor = jax.random.uniform(first, (NZ, width, width), jnp.float32, -math.sqrt(3.0), math.sqrt(3.0))
    shift = jnp.exp(jax.random.uniform(second, (NZ, 1, 1), jnp.float32, math.log(0.5), math.log(2.0)))
    matrix = jnp.einsum('mab,mcb->mac', factor, factor) / width + shift * jnp.eye(width, dtype=jnp.float32)
    return matrix


def draw_inner_inv(key, part):
    first, second = jax.random.split(jax.random.fold_in(key, 23), 2)
    width = (P_SIZE - 1) ** 2
    factor = jax.random.uniform(first, (NZ, width, width), jnp.float32, -math.sqrt(3.0), math.sqrt(3.0))
    shift = jax.random.uniform(second, (NZ, 1, 1), jnp.float32, 0.5, 1.5)
    return jnp.einsum('mab,mcb->mac', factor, factor) / width + shift * jnp.eye(width, dtype=jnp.float32)


def draw_element_cell(key, part):
    keys = jax.random.split(jax.random.fold_in(key, 37), ELEMENTS // EL_DEV)
    orders = jax.vmap(lambda single: jax.random.permutation(single, EL_DEV))(keys)
    return orders.reshape(-1).astype(jnp.int32)


def level_of(stream_key, extent, pieces, least, high):
    def one(position, shards_of):
        heights = jax.random.uniform(jax.random.fold_in(jax.random.fold_in(stream_key, 6), position), (shards_of,), jnp.float32, least / len(pieces), high / len(pieces))
        return jnp.repeat(jnp.exp(heights), extent[position] // shards_of).reshape((-1,) + (1,) * (len(extent) - position - 1))

    factor_of = one(*pieces[0])
    for cut in pieces[1:]:
        factor_of = factor_of * one(*cut)
    return factor_of


def normal_values(own_key, dims, scale, limit, pieces=(), kind=jnp.bfloat16):
    drawn = jax.random.normal(own_key, dims, jnp.float32) * scale
    if len(pieces) > 0:
        drawn = level_of(own_key, dims, pieces, -0.22, 0.18) * drawn
    return jnp.clip(drawn, min=-limit, max=limit).astype(kind)


def setup_inputs(seed: int = 0) -> dict:
    arg_keys = jax.random.split(jax.random.key(seed), 7)
    forcing = normal_values(arg_keys[0], (NZ, NODES, ELEMENTS), 1.0, 6.0, ((0, 2), (2, 16)), jnp.float32)
    element_coef = jnp.clip(jnp.exp(math.log(2.0) - 1.3862944 * jax.random.uniform(arg_keys[1], (ELEMENTS,), jnp.float32) ** level_of(arg_keys[1], (ELEMENTS,), ((0, 16),), -0.2, 0.2)), 0.5, 2.0)
    schur = draw_schur(jax.random.fold_in(arg_keys[6], 71), 0)
    couple = normal_values(arg_keys[3], (NZ, NB, NI), NI ** -0.5, 0.875, ((0, 2),), jnp.float32)
    inner_inv = draw_inner_inv(jax.random.fold_in(arg_keys[6], 71), 0)
    element_cell = draw_element_cell(jax.random.fold_in(arg_keys[6], 71), 0)
    return {"forcing": forcing, "element_coef": element_coef, "schur": schur, "couple": couple, "inner_inv": inner_inv, "element_cell": element_cell}


def dft_rows(length):
    row_index = jnp.arange(length)[:, None]
    plane_pos = jnp.arange(length, dtype=jnp.float32)[None, :]
    waves = ((row_index + 1) // 2).astype(jnp.float32)
    angles = 2.0 * math.pi * waves * plane_pos / length
    factor = math.sqrt(2.0 / length)
    result = jnp.where(row_index % 2 == 1, factor * jnp.cos(angles), factor * jnp.sin(angles))
    result = jnp.where(row_index == 0, 1.0 / math.sqrt(length), result)
    result = jnp.where(row_index == length - 1, jnp.cos(math.pi * plane_pos) / math.sqrt(length), result)
    return result.astype(jnp.float32)

def node_masks(row_ids, col_ids, rows_total, cols_total):
    slots = np.arange(4 * P_SIZE)
    on_left = jnp.asarray((slots == 0) | (slots >= 3 * P_SIZE))[:, None, None]
    on_right = jnp.asarray((slots >= P_SIZE) & (slots <= 2 * P_SIZE))[:, None, None]
    on_bottom = jnp.asarray(slots <= P_SIZE)[:, None, None]
    on_top = jnp.asarray((slots >= 2 * P_SIZE) & (slots <= 3 * P_SIZE))[:, None, None]
    dropped = on_left & (row_ids == 0)[None, :, None] | on_right & (row_ids == rows_total - 1)[None, :, None]
    dropped = dropped | on_bottom & (col_ids == 0)[None, None, :] | on_top & (col_ids == cols_total - 1)[None, None, :]
    keep = jnp.where(dropped, 0.0, 1.0).astype(jnp.float32)
    corner_weight = jnp.asarray(np.where(slots % P_SIZE == 0, 0.25, 0.5)).astype(jnp.float32)
    return (keep, keep * corner_weight[:, None, None])

def side_lines(values):
    return (jnp.concatenate([values[:, 0:1], values[:, 4 * P_SIZE - 1:3 * P_SIZE - 1:-1]], 1), values[:, P_SIZE:2 * P_SIZE + 1])

def add_sides(values, left_next, right_prev):
    blank = jnp.zeros((values.shape[0], P_SIZE - 1) + values.shape[2:], values.dtype)
    return values + jnp.concatenate([right_prev[:, 0:1], blank, left_next, blank, right_prev[:, P_SIZE:0:-1]], 1)

def end_lines(values):
    return (values[:, 0:P_SIZE + 1], values[:, 3 * P_SIZE:2 * P_SIZE - 1:-1])

def add_ends(values, bottom_next, top_prev):
    blank = jnp.zeros((values.shape[0], P_SIZE - 1) + values.shape[2:], values.dtype)
    return values + jnp.concatenate([top_prev, blank, bottom_next[:, ::-1], blank], 1)

def assemble(values):
    left_line, right_line = side_lines(values)
    left_next = jnp.pad(left_line[:, :, 1:], ((0, 0), (0, 0), (0, 1), (0, 0)))
    right_prev = jnp.pad(right_line[:, :, :-1], ((0, 0), (0, 0), (1, 0), (0, 0)))
    values = add_sides(values, left_next, right_prev)
    bottom_line, top_line = end_lines(values)
    bottom_next = jnp.pad(bottom_line[:, :, :, 1:], ((0, 0), (0, 0), (0, 0), (0, 1)))
    top_prev = jnp.pad(top_line[:, :, :, :-1], ((0, 0), (0, 0), (0, 0), (1, 0)))
    return add_ends(values, bottom_next, top_prev)

def reference(forcing, element_coef, schur, couple, inner_inv, element_cell):
    highest = lax.Precision.HIGHEST
    dft_table = dft_rows(NZ)
    spectral = jnp.einsum('jz,zne->jne', dft_table, forcing, precision=highest)
    block_ids = jnp.arange(ELEMENTS, dtype=jnp.int32) // EL_DEV
    grid_row = block_ids // N_EY * ELX + element_cell // ELY
    grid_col = block_ids % N_EY * ELY + element_cell % ELY
    location = (grid_row * NYE + grid_col).astype(jnp.int32)
    ordering = jnp.zeros((ELEMENTS,), jnp.int32).at[location].set(jnp.arange(ELEMENTS, dtype=jnp.int32))
    gridded = jnp.take(spectral, ordering, axis=2).reshape(NZ, NODES, NXE, NYE)
    scaling = jnp.take(element_coef, ordering).reshape(NXE, NYE)
    keep, weights = node_masks(jnp.arange(NXE), jnp.arange(NYE), NXE, NYE)

    def solve_mode(packed):
        fields, schur_mode, couple_mode, inner_mode = packed
        cycle_part = fields[:, :NB]
        inner_part = fields[:, NB:]
        condensed = cycle_part - jnp.einsum('mbi,mixy->mbxy', couple_mode, inner_part, precision=highest)
        residual = keep * assemble(condensed)

        def operator(search):
            return keep * assemble(scaling * jnp.einsum('mab,mbxy->maxy', schur_mode, search, precision=highest))

        def inner_sum(first, second):
            return lax.optimization_barrier(jnp.sum(weights * first * second, axis=(1, 2, 3)))[:, None, None, None]
        iterate = jnp.zeros_like(residual)
        search = residual
        norm_now = inner_sum(residual, residual)
        for sweep in range(ITERS):
            images = operator(search)
            step_size = norm_now / inner_sum(search, images)
            iterate = iterate + step_size * search
            residual = residual - step_size * images
            norm_next = inner_sum(residual, residual)
            search = residual + norm_next / norm_now * search
            norm_now = norm_next
        interior = jnp.einsum('mij,mjxy->mixy', inner_mode, inner_part, precision=highest) / scaling
        interior = interior - jnp.einsum('mbi,mbxy->mixy', couple_mode, iterate, precision=highest)
        return jnp.concatenate([iterate, interior], 1)
    modal = lax.map(solve_mode, (gridded[:, None], schur[:, None], couple[:, None], inner_inv[:, None]))
    modal = jnp.take(modal.reshape(NZ, NODES, ELEMENTS), location, axis=2)
    return jnp.einsum('jz,jne->zne', dft_table, modal, precision=highest)
```

```python
import math

import jax
import jax.numpy as jnp
import numpy as np
from jax import lax
from jax.sharding import PartitionSpec as P

P_SIZE = 8
ITERS = 3
ELX = 8
ELY = 16
NB = 4 * P_SIZE
HIGH = lax.Precision.HIGH
HIGHEST = lax.Precision.HIGHEST


def dft_rows(length):
    row_index = jnp.arange(length)[:, None]
    plane_pos = jnp.arange(length, dtype=jnp.float32)[None, :]
    waves = ((row_index + 1) // 2).astype(jnp.float32)
    angles = 2.0 * math.pi * waves * plane_pos / length
    factor = math.sqrt(2.0 / length)
    result = jnp.where(row_index % 2 == 1, factor * jnp.cos(angles), factor * jnp.sin(angles))
    result = jnp.where(row_index == 0, 1.0 / math.sqrt(length), result)
    result = jnp.where(
        row_index == length - 1, jnp.cos(math.pi * plane_pos) / math.sqrt(length), result
    )
    return result


def node_masks():
    slots = np.arange(NB)[:, None]
    cells = jnp.arange(ELX * ELY)[None, :]
    row_ids = lax.axis_index("ex") * ELX + cells // ELY
    col_ids = lax.axis_index("ey") * ELY + cells % ELY
    rows_total = ELX * lax.axis_size("ex")
    cols_total = ELY * lax.axis_size("ey")
    on_left = jnp.asarray((slots == 0) | (slots >= 3 * P_SIZE))
    on_right = jnp.asarray((slots >= P_SIZE) & (slots <= 2 * P_SIZE))
    on_bottom = jnp.asarray(slots <= P_SIZE)
    on_top = jnp.asarray((slots >= 2 * P_SIZE) & (slots <= 3 * P_SIZE))
    dropped = (
        on_left & (row_ids == 0)
        | on_right & (row_ids == rows_total - 1)
        | on_bottom & (col_ids == 0)
        | on_top & (col_ids == cols_total - 1)
    )
    keep = jnp.where(dropped, 0.0, 1.0).astype(jnp.float32)
    corner_weight = jnp.asarray(np.where(slots % P_SIZE == 0, 0.25, 0.5).astype(np.float32))
    return keep, keep * corner_weight


def shift_pair(axis):
    count = lax.axis_size(axis)
    forward = [(i, i + 1) for i in range(count - 1)]
    return forward, [(b, a) for a, b in forward]


def assemble(values):
    modes = values.shape[0]
    forward, backward = shift_pair("ex")
    left = jnp.concatenate([values[:, 0:1], values[:, NB - 1 : 3 * P_SIZE - 1 : -1]], 1)
    right = values[:, P_SIZE : 2 * P_SIZE + 1]
    low = lax.ppermute(right[:, :, -ELY:], "ex", forward)
    high = lax.ppermute(left[:, :, :ELY], "ex", backward)
    left_next = jnp.concatenate([left[:, :, ELY:], high], 2)
    right_prev = jnp.concatenate([low, right[:, :, :-ELY]], 2)
    blank = jnp.zeros((modes, P_SIZE - 1, values.shape[2]), values.dtype)
    values = values + jnp.concatenate(
        [right_prev[:, 0:1], blank, left_next, blank, right_prev[:, P_SIZE:0:-1]], 1
    )
    forward, backward = shift_pair("ey")
    bottom = values[:, 0 : P_SIZE + 1]
    top = values[:, 3 * P_SIZE : 2 * P_SIZE - 1 : -1]
    low = lax.ppermute(top[:, :, ELY - 1 :: ELY], "ey", forward)
    high = lax.ppermute(bottom[:, :, 0::ELY], "ey", backward)
    column = jnp.arange(ELX * ELY) % ELY
    bottom_next = jnp.where(
        column == ELY - 1, jnp.repeat(high, ELY, axis=2), jnp.roll(bottom, -1, axis=2)
    )
    top_prev = jnp.where(column == 0, jnp.repeat(low, ELY, axis=2), jnp.roll(top, 1, axis=2))
    return values + jnp.concatenate([top_prev, blank, bottom_next[:, ::-1], blank], 1)


def conjugate_gradients(condensed, schur, scaling):
    keep, weights = node_masks()

    def operator(search):
        return keep * assemble(
            scaling * jnp.einsum("mab,mbc->mac", schur, search, precision=HIGH)
        )

    def paired(vector, applied):
        return lax.psum(
            jnp.stack(
                [
                    jnp.sum(weights * vector * vector, axis=(1, 2)),
                    jnp.sum(weights * vector * applied, axis=(1, 2)),
                ]
            ),
            ("ex", "ey"),
        )

    def spread(scalars):
        return scalars[:, None, None]

    residual = keep * assemble(condensed)
    iterate = jnp.zeros_like(residual)
    applied = operator(residual)
    norm_now, curve_now = paired(residual, applied)
    step_size = norm_now / curve_now
    search = residual
    along_dir = applied
    for sweep in range(ITERS):
        iterate = iterate + spread(step_size) * search
        if sweep + 1 < ITERS:
            residual = residual - spread(step_size) * along_dir
            applied = operator(residual)
            norm_next, curve_now = paired(residual, applied)
            conj_ratio = norm_next / norm_now
            step_size = norm_next / (curve_now - conj_ratio * norm_next / step_size)
            search = residual + spread(conj_ratio) * search
            along_dir = applied + spread(conj_ratio) * along_dir
            norm_now = norm_next
    return iterate


def on_device(forcing, element_coef, schur, couple, inner_inv, element_cell):
    modes_dev = schur.shape[0]
    planes_dev = forcing.shape[0]
    elements = forcing.shape[2]
    groups = lax.axis_size("fourier")
    me = lax.axis_index("fourier")
    dft_table = dft_rows(modes_dev * groups)
    swap = [[(i, (i + hop) % groups) for i in range(groups)] for hop in range(groups)]
    plane_of = lambda group: lax.dynamic_slice_in_dim(dft_table, group * planes_dev, planes_dev, 1)
    rows_of = lambda table, group: lax.dynamic_slice_in_dim(table, group * modes_dev, modes_dev, 0)

    own_planes = plane_of(me)
    one_hot = (element_cell[:, None] == jnp.arange(elements)[None, :]).astype(jnp.float32)
    scaling = jnp.einsum("e,ec->c", element_coef, one_hot, precision=HIGHEST)

    order = [(me - hop) % groups for hop in range(groups)]
    couples = [couple] + [lax.ppermute(couple, "fourier", swap[h]) for h in range(1, groups)]

    partial = []
    condensed = None
    for hop in range(groups):
        spec = jnp.einsum(
            "mz,zne->mne", rows_of(own_planes, order[hop]), forcing, precision=HIGH
        )
        partial.append(spec[:, NB:])
        term = spec[:, :NB] - jnp.einsum("mbi,mie->mbe", couples[hop], spec[:, NB:], precision=HIGH)
        if hop:
            term = lax.ppermute(term, "fourier", [(b, a) for a, b in swap[hop]])
        condensed = term if condensed is None else condensed + term

    condensed = jnp.einsum("mbe,ec->mbc", condensed, one_hot, precision=HIGH)
    iterate = conjugate_gradients(condensed, schur, scaling)
    iterate = jnp.einsum("mbc,ec->mbe", iterate, one_hot, precision=HIGH)

    inner_forcing = forcing[:, NB:]
    others = [None] + [lax.ppermute(inner_forcing, "fourier", swap[h]) for h in range(1, groups)]
    velocity = None
    for hop in range(groups):
        inverse = lax.ppermute(inner_inv, "fourier", swap[hop]) if hop else inner_inv
        cycle = lax.ppermute(iterate, "fourier", swap[hop]) if hop else iterate
        inner = partial[hop]
        for far in range(1, groups):
            inner = inner + jnp.einsum(
                "mz,zne->mne",
                rows_of(plane_of(order[far]), order[hop]),
                others[far],
                precision=HIGH,
            )
        interior = jnp.einsum("mij,mje->mie", inverse, inner, precision=HIGH) / element_coef
        interior = interior - jnp.einsum("mbi,mbe->mie", couples[hop], cycle, precision=HIGH)
        term = jnp.einsum(
            "mz,mne->zne",
            rows_of(own_planes, order[hop]),
            jnp.concatenate([cycle, interior], 1),
            precision=HIGH,
        )
        velocity = term if velocity is None else velocity + term
    return velocity


def solution(mesh):
    placed = (
        P("fourier", None, ("ex", "ey")),
        P(("ex", "ey")),
        P("fourier", None, None),
        P("fourier", None, None),
        P("fourier", None, None),
        P(("ex", "ey")),
    )
    return jax.shard_map(
        on_device,
        mesh=mesh,
        in_specs=placed,
        out_specs=P("fourier", None, ("ex", "ey")),
        check_vma=False,
    )
```

```python
import functools
import math

import jax
import jax.numpy as jnp
import numpy as np
from jax import lax
from jax.experimental import pallas as pl
from jax.experimental.pallas import tpu as pltpu
from jax.sharding import PartitionSpec as P

P_SIZE = 8
ITERS = 3
ELX = 8
ELY = 16
NB = 4 * P_SIZE
HIGH = lax.Precision.HIGH
HIGHEST = lax.Precision.HIGHEST


def dft_rows(length):
    row_index = jnp.arange(length)[:, None]
    plane_pos = jnp.arange(length, dtype=jnp.float32)[None, :]
    waves = ((row_index + 1) // 2).astype(jnp.float32)
    angles = 2.0 * math.pi * waves * plane_pos / length
    factor = math.sqrt(2.0 / length)
    result = jnp.where(row_index % 2 == 1, factor * jnp.cos(angles), factor * jnp.sin(angles))
    result = jnp.where(row_index == 0, 1.0 / math.sqrt(length), result)
    result = jnp.where(
        row_index == length - 1, jnp.cos(math.pi * plane_pos) / math.sqrt(length), result
    )
    return result


def node_masks():
    slots = np.arange(NB)[:, None]
    cells = jnp.arange(ELX * ELY)[None, :]
    row_ids = lax.axis_index("ex") * ELX + cells // ELY
    col_ids = lax.axis_index("ey") * ELY + cells % ELY
    rows_total = ELX * lax.axis_size("ex")
    cols_total = ELY * lax.axis_size("ey")
    on_left = jnp.asarray((slots == 0) | (slots >= 3 * P_SIZE))
    on_right = jnp.asarray((slots >= P_SIZE) & (slots <= 2 * P_SIZE))
    on_bottom = jnp.asarray(slots <= P_SIZE)
    on_top = jnp.asarray((slots >= 2 * P_SIZE) & (slots <= 3 * P_SIZE))
    dropped = (
        on_left & (row_ids == 0)
        | on_right & (row_ids == rows_total - 1)
        | on_bottom & (col_ids == 0)
        | on_top & (col_ids == cols_total - 1)
    )
    keep = jnp.where(dropped, 0.0, 1.0).astype(jnp.float32)
    corner_weight = jnp.asarray(np.where(slots % P_SIZE == 0, 0.25, 0.5).astype(np.float32))
    return keep, keep * corner_weight


def split_high_low(values):
    high = lax.reduce_precision(values, 8, 7)
    return high.astype(jnp.bfloat16), (values - high).astype(jnp.bfloat16)


def cg_kernel(
    modes,
    cond_ref,
    schur_ref,
    scale_ref,
    keep_ref,
    weight_ref,
    x_ref,
    res_ref,
    app_ref,
    dir_ref,
    along_ref,
    xs_ref,
    xr_ref,
    ys_ref,
    yr_ref,
    ps_ref,
    pr_ex,
    pr_ey,
    halo_send,
    halo_recv,
    sum_send_ex,
    sum_recv_ex,
    sum_send_ey,
    sum_recv_ey,
):
    cells = cond_ref.shape[1]
    sizes = {axis: lax.axis_size(axis) for axis in ("ex", "ey")}
    place = {axis: lax.axis_index(axis) for axis in ("ex", "ey")}
    lane = lax.broadcasted_iota(jnp.int32, (modes, cells), 1)
    lane_row = lane // ELY
    lane_col = lane % ELY

    def node(n):
        if isinstance(n, int):
            return pl.ds(n * modes, modes)
        return pl.ds(pl.multiple_of(n * modes, modes), modes)

    def turned(value, shift):
        shift = shift % cells
        return pltpu.roll(value, shift, 1) if shift else value

    xr_ref[...] = jnp.zeros_like(xr_ref)
    yr_ref[...] = jnp.zeros_like(yr_ref)

    barrier = pltpu.get_barrier_semaphore()
    for axis in ("ex", "ey"):
        for hop in range(1, sizes[axis]):
            pl.semaphore_signal(
                barrier,
                inc=1,
                device_id={axis: lax.rem(place[axis] + hop, sizes[axis])},
                device_id_type=pl.DeviceIdType.MESH,
            )
    pl.semaphore_wait(barrier, sizes["ex"] + sizes["ey"] - 2)

    def halo_copies(axis, send, recv, turn):
        index = 2 * (axis == "ey")
        up, down = [
            pltpu.make_async_remote_copy(
                src_ref=send.at[turn, way],
                dst_ref=recv.at[turn, way],
                send_sem=halo_send.at[turn, index + way],
                recv_sem=halo_recv.at[turn, index + way],
                device_id={axis: lax.rem(place[axis] + step + sizes[axis], sizes[axis])},
                device_id_type=pl.DeviceIdType.MESH,
            )
            for way, step in ((0, 1), (1, -1))
        ]
        has_next = place[axis] < sizes[axis] - 1
        has_prev = place[axis] > 0

        def start():
            pl.when(has_next)(up.start)
            pl.when(has_prev)(down.start)

        def arrive():
            pl.when(has_prev)(up.wait_recv)
            pl.when(has_next)(down.wait_recv)

        def leave():
            pl.when(has_next)(up.wait_send)
            pl.when(has_prev)(down.wait_send)

        return start, arrive, leave

    def assemble(ref, turn):
        left = lambda k: (NB - k) % NB
        right = lambda k: P_SIZE + k
        last = cells - ELY
        up = jnp.zeros((modes, cells), jnp.float32)
        down = up
        for k in range(P_SIZE):
            up = jnp.where(lane_row == k, turned(ref[node(right(k)), :], ELY * k - last), up)
            down = jnp.where(lane_row == k, turned(ref[node(left(k)), :], ELY * k), down)
        xs_ref[turn, 0, 0] = up
        xs_ref[turn, 1, 0] = down
        xs_ref[turn, 0, 1] = turned(ref[node(right(P_SIZE)), :], -last)
        xs_ref[turn, 1, 1] = ref[node(left(P_SIZE)), :]
        start, arrive, leave = halo_copies("ex", xs_ref, xr_ref, turn)
        start()
        arrive()
        for k in range(P_SIZE + 1):
            part, lanes = divmod(k, P_SIZE)
            low = turned(xr_ref[turn, 0, part], -ELY * lanes)
            high = turned(xr_ref[turn, 1, part], last - ELY * lanes)
            here_left, here_right = ref[node(left(k)), :], ref[node(right(k)), :]
            ref[node(left(k)), :] = here_left + jnp.where(
                lane_row == 0, low, turned(here_right, ELY)
            )
            ref[node(right(k)), :] = here_right + jnp.where(
                lane_row == ELX - 1, high, turned(here_left, -ELY)
            )
        leave()

        bottom = lambda k: k
        top = lambda k: 3 * P_SIZE - k
        up = jnp.zeros((modes, cells), jnp.float32)
        down = up
        for k in range(P_SIZE + 1):
            up = jnp.where(lane_col == k, turned(ref[node(top(k)), :], k - ELY + 1), up)
            down = jnp.where(lane_col == k, turned(ref[node(bottom(k)), :], k), down)
        ys_ref[turn, 0] = up
        ys_ref[turn, 1] = down
        start, arrive, leave = halo_copies("ey", ys_ref, yr_ref, turn)
        start()
        for n in list(range(P_SIZE + 1, 2 * P_SIZE)) + list(range(3 * P_SIZE + 1, NB)):
            ref[node(n), :] = ref[node(n), :] * keep_ref[n : n + 1, :]
        arrive()
        low_all = yr_ref[turn, 0]
        high_all = yr_ref[turn, 1]
        for k in range(P_SIZE + 1):
            b, t = bottom(k), top(k)
            here_bottom, here_top = ref[node(b), :], ref[node(t), :]
            ref[node(b), :] = keep_ref[b : b + 1, :] * (
                here_bottom
                + jnp.where(lane_col == 0, turned(low_all, -k), turned(here_top, 1))
            )
            ref[node(t), :] = keep_ref[t : t + 1, :] * (
                here_top
                + jnp.where(
                    lane_col == ELY - 1, turned(high_all, ELY - 1 - k), turned(here_bottom, -1)
                )
            )
        leave()

    def operator(turn):
        scale = scale_ref[0:1, :]
        block = 8

        def step(outer, carry):
            for inner in range(block):
                mode = outer * block + inner
                value = res_ref[pl.ds(mode, NB, stride=modes), :]
                high = value.astype(jnp.bfloat16)
                low = (value - high.astype(jnp.float32)).astype(jnp.bfloat16)
                image = jnp.dot(
                    schur_ref[mode],
                    jnp.concatenate([high, low, high], 0),
                    preferred_element_type=jnp.float32,
                )
                app_ref[pl.ds(mode, NB, stride=modes), :] = image * scale
            return carry

        lax.fori_loop(0, modes // block, step, 0)
        assemble(app_ref, turn)

    def group_sum(mine, axis, turn, stage, slots, send_sem, recv_sem):
        ps_ref[turn, stage] = mine
        copies = [
            pltpu.make_async_remote_copy(
                src_ref=ps_ref.at[turn, stage],
                dst_ref=slots.at[turn, hop - 1],
                send_sem=send_sem.at[turn, hop - 1],
                recv_sem=recv_sem.at[turn, hop - 1],
                device_id={axis: lax.rem(place[axis] + hop, sizes[axis])},
                device_id_type=pl.DeviceIdType.MESH,
            )
            for hop in range(1, sizes[axis])
        ]
        for copy in copies:
            copy.start()
        for hop, copy in enumerate(copies):
            copy.wait_recv()
            mine = mine + slots[turn, hop]
        for copy in copies:
            copy.wait_send()
        return mine

    def paired(turn):
        def step(n, sums):
            weighted = weight_ref[pl.ds(n, 1), :] * res_ref[node(n), :]
            return (
                sums[0] + weighted * res_ref[node(n), :],
                sums[1] + weighted * app_ref[node(n), :],
            )

        zero = jnp.zeros((modes, cells), jnp.float32)
        norm, curve = lax.fori_loop(0, NB, step, (zero, zero))
        total = lax.dot_general(
            jnp.ones((8, cells), jnp.float32),
            jnp.concatenate([norm, curve], 0),
            (((1,), (1,)), ((), ())),
            precision=HIGHEST,
            preferred_element_type=jnp.float32,
        )
        total = group_sum(total, "ey", turn, 0, pr_ey, sum_send_ey, sum_recv_ey)
        total = group_sum(total, "ex", turn, 1, pr_ex, sum_send_ex, sum_recv_ex)
        row = lax.broadcasted_iota(jnp.int32, (modes, 2 * modes), 0)
        column = lax.broadcasted_iota(jnp.int32, (modes, 2 * modes), 1)
        pick = lambda offset: jnp.sum(
            jnp.where(column == row + offset, total[0:1, :], 0.0), axis=1, keepdims=True
        )
        return pick(0), pick(modes)

    res_ref[...] = cond_ref[...]
    assemble(res_ref, 0)
    step_size = None
    for sweep in range(ITERS):
        operator(sweep + 1)
        norm_next, curve_now = paired(sweep)
        if sweep == 0:
            conj_ratio = None
            step_size = norm_next / curve_now
        else:
            conj_ratio = norm_next / norm_now
            step_size = norm_next / (curve_now - conj_ratio * norm_next / step_size)
        norm_now = norm_next

        def update(n, carry, sweep=sweep, conj_ratio=conj_ratio, step_size=step_size):
            rows = node(n)
            search = res_ref[rows, :]
            if sweep:
                search = search + conj_ratio * dir_ref[rows, :]
                x_ref[rows, :] = x_ref[rows, :] + step_size * search
            else:
                x_ref[rows, :] = step_size * search
            if sweep + 1 < ITERS:
                dir_ref[rows, :] = search
                along = app_ref[rows, :]
                if sweep:
                    along = along + conj_ratio * along_ref[rows, :]
                along_ref[rows, :] = along
                res_ref[rows, :] = res_ref[rows, :] - step_size * along
            return carry

        lax.fori_loop(0, NB, update, 0)


def conjugate_gradients(condensed, schur, scaling):
    modes, cells = condensed.shape[1:]
    keep, weights = node_masks()
    high, low = split_high_low(schur)
    stacked = jnp.concatenate([high, high, low], 2)
    field = pltpu.VMEM((NB * modes, cells), jnp.float32)
    along_ex, along_ey = lax.axis_size("ex") - 1, lax.axis_size("ey") - 1
    turns = ITERS + 1
    strips = lambda *lead: pltpu.VMEM(lead + (modes, cells), jnp.float32)
    tile = lambda *lead: pltpu.VMEM(lead + (8, 2 * modes), jnp.float32)
    semaphores = lambda *dims: pltpu.SemaphoreType.DMA(dims)
    whole = pl.BlockSpec(memory_space=pltpu.VMEM)
    solved = pl.pallas_call(
        functools.partial(cg_kernel, modes),
        out_shape=jax.ShapeDtypeStruct((NB * modes, cells), jnp.float32),
        in_specs=[whole] * 5,
        out_specs=whole,
        scratch_shapes=[field] * 4
        + [
            strips(turns, 2, 2),
            strips(turns, 2, 2),
            strips(turns, 2),
            strips(turns, 2),
            tile(ITERS, 2),
            tile(ITERS, along_ex),
            tile(ITERS, along_ey),
            semaphores(turns, 4),
            semaphores(turns, 4),
            semaphores(ITERS, along_ex),
            semaphores(ITERS, along_ex),
            semaphores(ITERS, along_ey),
            semaphores(ITERS, along_ey),
        ],
        compiler_params=pltpu.CompilerParams(
            collective_id=0, has_side_effects=True, vmem_limit_bytes=40 << 20
        ),
        cost_estimate=pl.CostEstimate(flops=10**9, bytes_accessed=10**8, transcendentals=0),
    )(condensed.reshape(NB * modes, cells), stacked, scaling[None], keep, weights)
    return solved.reshape(NB, modes, cells)


def on_device(forcing, element_coef, schur, couple, inner_inv, element_cell):
    modes_dev = schur.shape[0]
    planes_dev = forcing.shape[0]
    elements = forcing.shape[2]
    groups = lax.axis_size("fourier")
    me = lax.axis_index("fourier")
    dft_table = dft_rows(modes_dev * groups)
    swap = [[(i, (i + hop) % groups) for i in range(groups)] for hop in range(groups)]
    plane_of = lambda group: lax.dynamic_slice_in_dim(dft_table, group * planes_dev, planes_dev, 1)
    rows_of = lambda table, group: lax.dynamic_slice_in_dim(table, group * modes_dev, modes_dev, 0)

    own_planes = plane_of(me)
    one_hot = (element_cell[:, None] == jnp.arange(elements)[None, :]).astype(jnp.float32)
    scaling = jnp.einsum("e,ec->c", element_coef, one_hot, precision=HIGHEST)

    order = [(me - hop) % groups for hop in range(groups)]
    couples = [couple] + [lax.ppermute(couple, "fourier", swap[h]) for h in range(1, groups)]

    partial = []
    condensed = None
    for hop in range(groups):
        spec = jnp.einsum(
            "mz,zne->mne", rows_of(own_planes, order[hop]), forcing, precision=HIGH
        )
        partial.append(spec[:, NB:])
        term = spec[:, :NB] - jnp.einsum("mbi,mie->mbe", couples[hop], spec[:, NB:], precision=HIGH)
        if hop:
            term = lax.ppermute(term, "fourier", [(b, a) for a, b in swap[hop]])
        condensed = term if condensed is None else condensed + term

    condensed = jnp.einsum("mbe,ec->bmc", condensed, one_hot, precision=HIGH)
    iterate = conjugate_gradients(condensed, schur, scaling)
    iterate = jnp.einsum("bmc,ec->mbe", iterate, one_hot, precision=HIGH)

    inner_forcing = forcing[:, NB:]
    others = [None] + [lax.ppermute(inner_forcing, "fourier", swap[h]) for h in range(1, groups)]
    velocity = None
    for hop in range(groups):
        inverse = lax.ppermute(inner_inv, "fourier", swap[hop]) if hop else inner_inv
        cycle = lax.ppermute(iterate, "fourier", swap[hop]) if hop else iterate
        inner = partial[hop]
        for far in range(1, groups):
            inner = inner + jnp.einsum(
                "mz,zne->mne",
                rows_of(plane_of(order[far]), order[hop]),
                others[far],
                precision=HIGH,
            )
        interior = jnp.einsum("mij,mje->mie", inverse, inner, precision=HIGH) / element_coef
        interior = interior - jnp.einsum("mbi,mbe->mie", couples[hop], cycle, precision=HIGH)
        term = jnp.einsum(
            "mz,mne->zne",
            rows_of(own_planes, order[hop]),
            jnp.concatenate([cycle, interior], 1),
            precision=HIGH,
        )
        velocity = term if velocity is None else velocity + term
    return velocity


def solution(mesh):
    placed = (
        P("fourier", None, ("ex", "ey")),
        P(("ex", "ey")),
        P("fourier", None, None),
        P("fourier", None, None),
        P("fourier", None, None),
        P(("ex", "ey")),
    )
    return jax.shard_map(
        on_device,
        mesh=mesh,
        in_specs=placed,
        out_specs=P("fourier", None, ("ex", "ey")),
        check_vma=False,
    )
```

```python
import functools
import math

import jax
import jax.numpy as jnp
import numpy as np
from jax import lax
from jax.experimental import pallas as pl
from jax.experimental.pallas import tpu as pltpu
from jax.sharding import PartitionSpec as P

P_SIZE = 8
ITERS = 3
ELX = 8
ELY = 16
NB = 4 * P_SIZE
HIGH = lax.Precision.HIGH
HIGHEST = lax.Precision.HIGHEST


def dft_rows(length):
    row_index = jnp.arange(length)[:, None]
    plane_pos = jnp.arange(length, dtype=jnp.float32)[None, :]
    waves = ((row_index + 1) // 2).astype(jnp.float32)
    angles = 2.0 * math.pi * waves * plane_pos / length
    factor = math.sqrt(2.0 / length)
    result = jnp.where(row_index % 2 == 1, factor * jnp.cos(angles), factor * jnp.sin(angles))
    result = jnp.where(row_index == 0, 1.0 / math.sqrt(length), result)
    result = jnp.where(
        row_index == length - 1, jnp.cos(math.pi * plane_pos) / math.sqrt(length), result
    )
    return result


def node_masks():
    slots = np.arange(NB)[:, None]
    cells = jnp.arange(ELX * ELY)[None, :]
    row_ids = lax.axis_index("ex") * ELX + cells // ELY
    col_ids = lax.axis_index("ey") * ELY + cells % ELY
    rows_total = ELX * lax.axis_size("ex")
    cols_total = ELY * lax.axis_size("ey")
    on_left = jnp.asarray((slots == 0) | (slots >= 3 * P_SIZE))
    on_right = jnp.asarray((slots >= P_SIZE) & (slots <= 2 * P_SIZE))
    on_bottom = jnp.asarray(slots <= P_SIZE)
    on_top = jnp.asarray((slots >= 2 * P_SIZE) & (slots <= 3 * P_SIZE))
    dropped = (
        on_left & (row_ids == 0)
        | on_right & (row_ids == rows_total - 1)
        | on_bottom & (col_ids == 0)
        | on_top & (col_ids == cols_total - 1)
    )
    keep = jnp.where(dropped, 0.0, 1.0).astype(jnp.float32)
    corner_weight = jnp.asarray(np.where(slots % P_SIZE == 0, 0.25, 0.5).astype(np.float32))
    return keep, keep * corner_weight


def split_high_low(values):
    high = lax.reduce_precision(values, 8, 7)
    return high.astype(jnp.bfloat16), (values - high).astype(jnp.bfloat16)


def cg_kernel(
    modes,
    cond_ref,
    schur_ref,
    scale_ref,
    keep_ref,
    weight_ref,
    x_ref,
    res_ref,
    app_ref,
    dir_ref,
    along_ref,
    xs_ref,
    xr_ref,
    ys_ref,
    yr_ref,
    ps_ref,
    pr_ex,
    pr_ey,
    halo_send,
    halo_recv,
    sum_send_ex,
    sum_recv_ex,
    sum_send_ey,
    sum_recv_ey,
):
    cells = cond_ref.shape[1]
    sizes = {axis: lax.axis_size(axis) for axis in ("ex", "ey")}
    place = {axis: lax.axis_index(axis) for axis in ("ex", "ey")}
    lane = lax.broadcasted_iota(jnp.int32, (modes, cells), 1)
    lane_row = lane // ELY
    lane_col = lane % ELY

    def node(n):
        if isinstance(n, int):
            return pl.ds(n * modes, modes)
        return pl.ds(pl.multiple_of(n * modes, modes), modes)

    def turned(value, shift):
        shift = shift % cells
        return pltpu.roll(value, shift, 1) if shift else value

    xr_ref[...] = jnp.zeros_like(xr_ref)
    yr_ref[...] = jnp.zeros_like(yr_ref)

    barrier = pltpu.get_barrier_semaphore()
    for axis in ("ex", "ey"):
        for hop in range(1, sizes[axis]):
            pl.semaphore_signal(
                barrier,
                inc=1,
                device_id={axis: lax.rem(place[axis] + hop, sizes[axis])},
                device_id_type=pl.DeviceIdType.MESH,
            )
    for ex_step in (1, -1):
        for ey_step in (1, -1):
            pl.semaphore_signal(
                barrier,
                inc=1,
                device_id={
                    "ex": lax.rem(place["ex"] + ex_step + sizes["ex"], sizes["ex"]),
                    "ey": lax.rem(place["ey"] + ey_step + sizes["ey"], sizes["ey"]),
                },
                device_id_type=pl.DeviceIdType.MESH,
            )
    pl.semaphore_wait(barrier, sizes["ex"] + sizes["ey"] + 2)

    def exists(axis, step):
        if step == 0:
            return None
        return place[axis] < sizes[axis] - 1 if step > 0 else place[axis] > 0

    def guarded(ex_step, ey_step, action):
        tests = [t for t in (exists("ex", ex_step), exists("ey", ey_step)) if t is not None]
        pl.when(functools.reduce(jnp.logical_and, tests))(action)

    def halo_copy(turn, number, source, target, ex_step, ey_step):
        copy = pltpu.make_async_remote_copy(
            src_ref=source,
            dst_ref=target,
            send_sem=halo_send.at[turn, number],
            recv_sem=halo_recv.at[turn, number],
            device_id={
                "ex": lax.rem(place["ex"] + ex_step + sizes["ex"], sizes["ex"]),
                "ey": lax.rem(place["ey"] + ey_step + sizes["ey"], sizes["ey"]),
            },
            device_id_type=pl.DeviceIdType.MESH,
        )
        guarded(ex_step, ey_step, copy.start)

        def arrive():
            guarded(-ex_step, -ey_step, copy.wait_recv)

        def leave():
            guarded(ex_step, ey_step, copy.wait_send)

        return arrive, leave

    def assemble(ref, turn):
        bottom = lambda k: k
        top = lambda k: 3 * P_SIZE - k
        up = jnp.zeros((modes, cells), jnp.float32)
        down = up
        for k in range(P_SIZE + 1):
            up = jnp.where(lane_col == k, turned(ref[node(top(k)), :], k - ELY + 1), up)
            down = jnp.where(lane_col == k, turned(ref[node(bottom(k)), :], k), down)
        ys_ref[turn, 0] = up
        ys_ref[turn, 1] = down
        copies = []
        for slot, ex_step in ((1, 1), (2, -1), (0, 0)):
            for way, ey_step in ((0, 1), (1, -1)):
                copies.append(
                    halo_copy(
                        turn,
                        2 * slot + way,
                        ys_ref.at[turn, way],
                        yr_ref.at[turn, slot, way],
                        ex_step,
                        ey_step,
                    )
                )

        left = lambda k: (NB - k) % NB
        right = lambda k: P_SIZE + k
        last = cells - ELY
        up = jnp.zeros((modes, cells), jnp.float32)
        down = up
        for k in range(P_SIZE):
            up = jnp.where(lane_row == k, turned(ref[node(right(k)), :], ELY * k - last), up)
            down = jnp.where(lane_row == k, turned(ref[node(left(k)), :], ELY * k), down)
        xs_ref[turn, 0, 0] = up
        xs_ref[turn, 1, 0] = down
        xs_ref[turn, 0, 1] = turned(ref[node(right(P_SIZE)), :], -last)
        xs_ref[turn, 1, 1] = ref[node(left(P_SIZE)), :]
        for way, ex_step in ((0, 1), (1, -1)):
            copies.append(
                halo_copy(turn, 6 + way, xs_ref.at[turn, way], xr_ref.at[turn, way], ex_step, 0)
            )

        for k in range(P_SIZE + 1):
            here_left, here_right = ref[node(left(k)), :], ref[node(right(k)), :]
            ref[node(left(k)), :] = here_left + jnp.where(
                lane_row == 0, 0.0, turned(here_right, ELY)
            )
            ref[node(right(k)), :] = here_right + jnp.where(
                lane_row == ELX - 1, 0.0, turned(here_left, -ELY)
            )
        for arrive, _ in copies:
            arrive()

        for k in range(P_SIZE + 1):
            part, lanes = divmod(k, P_SIZE)
            low = turned(xr_ref[turn, 0, part], -ELY * lanes)
            high = turned(xr_ref[turn, 1, part], last - ELY * lanes)
            for n, halo, row in ((left(k), low, 0), (right(k), high, ELX - 1)):
                value = ref[node(n), :] + jnp.where(lane_row == row, halo, 0.0)
                if n % (2 * P_SIZE) > P_SIZE:
                    value = value * keep_ref[n : n + 1, :]
                ref[node(n), :] = value

        lines = []
        for way in range(2):
            line = yr_ref[turn, 0, way]
            before = jnp.where(
                lane == 0, turned(yr_ref[turn, 1, way], P_SIZE), turned(line, P_SIZE)
            )
            after = jnp.where(
                lane == last + P_SIZE, turned(yr_ref[turn, 2, way], -P_SIZE), turned(line, -P_SIZE)
            )
            lines.append(
                line
                + jnp.where(lane_col == 0, before, jnp.where(lane_col == P_SIZE, after, 0.0))
            )
        low_all, high_all = lines
        for k in range(P_SIZE + 1):
            b, t = bottom(k), top(k)
            here_bottom, here_top = ref[node(b), :], ref[node(t), :]
            ref[node(b), :] = keep_ref[b : b + 1, :] * (
                here_bottom
                + jnp.where(lane_col == 0, turned(low_all, -k), turned(here_top, 1))
            )
            ref[node(t), :] = keep_ref[t : t + 1, :] * (
                here_top
                + jnp.where(
                    lane_col == ELY - 1, turned(high_all, ELY - 1 - k), turned(here_bottom, -1)
                )
            )
        for _, leave in copies:
            leave()

    def operator(turn):
        scale = scale_ref[0:1, :]
        block = 8

        def step(outer, carry):
            for inner in range(block):
                mode = outer * block + inner
                value = res_ref[pl.ds(mode, NB, stride=modes), :]
                high = value.astype(jnp.bfloat16)
                low = (value - high.astype(jnp.float32)).astype(jnp.bfloat16)
                image = jnp.dot(
                    schur_ref[mode],
                    jnp.concatenate([high, low, high], 0),
                    preferred_element_type=jnp.float32,
                )
                app_ref[pl.ds(mode, NB, stride=modes), :] = image * scale
            return carry

        lax.fori_loop(0, modes // block, step, 0)
        assemble(app_ref, turn)

    def group_sum(mine, axis, turn, stage, slots, send_sem, recv_sem):
        ps_ref[turn, stage] = mine
        copies = [
            pltpu.make_async_remote_copy(
                src_ref=ps_ref.at[turn, stage],
                dst_ref=slots.at[turn, hop - 1],
                send_sem=send_sem.at[turn, hop - 1],
                recv_sem=recv_sem.at[turn, hop - 1],
                device_id={axis: lax.rem(place[axis] + hop, sizes[axis])},
                device_id_type=pl.DeviceIdType.MESH,
            )
            for hop in range(1, sizes[axis])
        ]
        for copy in copies:
            copy.start()
        for hop, copy in enumerate(copies):
            copy.wait_recv()
            mine = mine + slots[turn, hop]
        for copy in copies:
            copy.wait_send()
        return mine

    def paired(turn):
        def step(n, sums):
            weighted = weight_ref[pl.ds(n, 1), :] * res_ref[node(n), :]
            return (
                sums[0] + weighted * res_ref[node(n), :],
                sums[1] + weighted * app_ref[node(n), :],
            )

        zero = jnp.zeros((modes, cells), jnp.float32)
        norm, curve = lax.fori_loop(0, NB, step, (zero, zero))
        total = lax.dot_general(
            jnp.ones((8, cells), jnp.float32),
            jnp.concatenate([norm, curve], 0),
            (((1,), (1,)), ((), ())),
            precision=HIGHEST,
            preferred_element_type=jnp.float32,
        )
        total = group_sum(total, "ey", turn, 0, pr_ey, sum_send_ey, sum_recv_ey)
        total = group_sum(total, "ex", turn, 1, pr_ex, sum_send_ex, sum_recv_ex)
        row = lax.broadcasted_iota(jnp.int32, (modes, 2 * modes), 0)
        column = lax.broadcasted_iota(jnp.int32, (modes, 2 * modes), 1)
        pick = lambda offset: jnp.sum(
            jnp.where(column == row + offset, total[0:1, :], 0.0), axis=1, keepdims=True
        )
        return pick(0), pick(modes)

    res_ref[...] = cond_ref[...]
    assemble(res_ref, 0)
    step_size = None
    for sweep in range(ITERS):
        operator(sweep + 1)
        norm_next, curve_now = paired(sweep)
        if sweep == 0:
            conj_ratio = None
            step_size = norm_next / curve_now
        else:
            conj_ratio = norm_next / norm_now
            step_size = norm_next / (curve_now - conj_ratio * norm_next / step_size)
        norm_now = norm_next

        def update(n, carry, sweep=sweep, conj_ratio=conj_ratio, step_size=step_size):
            rows = node(n)
            search = res_ref[rows, :]
            if sweep:
                search = search + conj_ratio * dir_ref[rows, :]
                x_ref[rows, :] = x_ref[rows, :] + step_size * search
            else:
                x_ref[rows, :] = step_size * search
            if sweep + 1 < ITERS:
                dir_ref[rows, :] = search
                along = app_ref[rows, :]
                if sweep:
                    along = along + conj_ratio * along_ref[rows, :]
                along_ref[rows, :] = along
                res_ref[rows, :] = res_ref[rows, :] - step_size * along
            return carry

        lax.fori_loop(0, NB, update, 0)


def conjugate_gradients(condensed, schur, scaling):
    modes, cells = condensed.shape[1:]
    keep, weights = node_masks()
    high, low = split_high_low(schur)
    stacked = jnp.concatenate([high, high, low], 2)
    field = pltpu.VMEM((NB * modes, cells), jnp.float32)
    along_ex, along_ey = lax.axis_size("ex") - 1, lax.axis_size("ey") - 1
    turns = ITERS + 1
    strips = lambda *lead: pltpu.VMEM(lead + (modes, cells), jnp.float32)
    tile = lambda *lead: pltpu.VMEM(lead + (8, 2 * modes), jnp.float32)
    semaphores = lambda *dims: pltpu.SemaphoreType.DMA(dims)
    whole = pl.BlockSpec(memory_space=pltpu.VMEM)
    solved = pl.pallas_call(
        functools.partial(cg_kernel, modes),
        out_shape=jax.ShapeDtypeStruct((NB * modes, cells), jnp.float32),
        in_specs=[whole] * 5,
        out_specs=whole,
        scratch_shapes=[field] * 4
        + [
            strips(turns, 2, 2),
            strips(turns, 2, 2),
            strips(turns, 2),
            strips(turns, 3, 2),
            tile(ITERS, 2),
            tile(ITERS, along_ex),
            tile(ITERS, along_ey),
            semaphores(turns, 8),
            semaphores(turns, 8),
            semaphores(ITERS, along_ex),
            semaphores(ITERS, along_ex),
            semaphores(ITERS, along_ey),
            semaphores(ITERS, along_ey),
        ],
        compiler_params=pltpu.CompilerParams(
            collective_id=0, has_side_effects=True, vmem_limit_bytes=40 << 20
        ),
        cost_estimate=pl.CostEstimate(flops=10**9, bytes_accessed=2 * 10**8, transcendentals=0),
    )(condensed.reshape(NB * modes, cells), stacked, scaling[None], keep, weights)
    return solved.reshape(NB, modes, cells)


def on_device(forcing, element_coef, schur, couple, inner_inv, element_cell):
    modes_dev = schur.shape[0]
    planes_dev = forcing.shape[0]
    elements = forcing.shape[2]
    groups = lax.axis_size("fourier")
    me = lax.axis_index("fourier")
    dft_table = dft_rows(modes_dev * groups)
    swap = [[(i, (i + hop) % groups) for i in range(groups)] for hop in range(groups)]
    plane_of = lambda group: lax.dynamic_slice_in_dim(dft_table, group * planes_dev, planes_dev, 1)
    rows_of = lambda table, group: lax.dynamic_slice_in_dim(table, group * modes_dev, modes_dev, 0)

    own_planes = plane_of(me)
    one_hot = (element_cell[:, None] == jnp.arange(elements)[None, :]).astype(jnp.float32)
    scaling = jnp.einsum("e,ec->c", element_coef, one_hot, precision=HIGHEST)

    order = [(me - hop) % groups for hop in range(groups)]
    couples = [couple] + [lax.ppermute(couple, "fourier", swap[h]) for h in range(1, groups)]

    partial = []
    condensed = None
    for hop in range(groups):
        spec = jnp.einsum(
            "mz,zne->mne", rows_of(own_planes, order[hop]), forcing, precision=HIGH
        )
        partial.append(spec[:, NB:])
        term = spec[:, :NB] - jnp.einsum("mbi,mie->mbe", couples[hop], spec[:, NB:], precision=HIGH)
        if hop:
            term = lax.ppermute(term, "fourier", [(b, a) for a, b in swap[hop]])
        condensed = term if condensed is None else condensed + term

    half, inner_count = modes_dev // 2, inner_inv.shape[2]
    padded = jnp.pad(inner_inv, ((0, 0), (0, 0), (0, elements // 2 - inner_count)))
    parcel = jnp.concatenate(
        [forcing[:, NB:], jnp.concatenate([padded[:half], padded[half:]], 2)], 0
    )
    condensed, parcel = lax.optimization_barrier((condensed, parcel))
    parcels = [None] + [lax.ppermute(parcel, "fourier", swap[h]) for h in range(1, groups)]
    condensed = jnp.einsum("mbe,ec->bmc", condensed, one_hot, precision=HIGH)
    iterate = conjugate_gradients(condensed, schur, scaling)
    iterate = jnp.einsum("bmc,ec->mbe", iterate, one_hot, precision=HIGH)

    velocity = None
    for hop in range(groups):
        inverse = inner_inv
        if hop:
            pairs = parcels[hop][planes_dev:]
            inverse = jnp.concatenate(
                [pairs[:, :, :inner_count], pairs[:, :, elements // 2 :][:, :, :inner_count]], 0
            )
        cycle = lax.ppermute(iterate, "fourier", swap[hop]) if hop else iterate
        inner = partial[hop]
        for far in range(1, groups):
            inner = inner + jnp.einsum(
                "mz,zne->mne",
                rows_of(plane_of(order[far]), order[hop]),
                parcels[far][:planes_dev],
                precision=HIGH,
            )
        interior = jnp.einsum("mij,mje->mie", inverse, inner, precision=HIGH) / element_coef
        interior = interior - jnp.einsum("mbi,mbe->mie", couples[hop], cycle, precision=HIGH)
        term = jnp.einsum(
            "mz,mne->zne",
            rows_of(own_planes, order[hop]),
            jnp.concatenate([cycle, interior], 1),
            precision=HIGH,
        )
        velocity = term if velocity is None else velocity + term
    return velocity


def solution(mesh):
    placed = (
        P("fourier", None, ("ex", "ey")),
        P(("ex", "ey")),
        P("fourier", None, None),
        P("fourier", None, None),
        P("fourier", None, None),
        P(("ex", "ey")),
    )
    return jax.shard_map(
        on_device,
        mesh=mesh,
        in_specs=placed,
        out_specs=P("fourier", None, ("ex", "ey")),
        check_vma=False,
    )
```

```python
import functools
import math

import jax
import jax.numpy as jnp
import numpy as np
from jax import lax
from jax.experimental import pallas as pl
from jax.experimental.pallas import tpu as pltpu
from jax.sharding import PartitionSpec as P

P_SIZE = 8
ITERS = 3
ELX = 8
ELY = 16
NB = 4 * P_SIZE
HIGH = lax.Precision.HIGH
HIGHEST = lax.Precision.HIGHEST


def dft_rows(length):
    row_index = jnp.arange(length)[:, None]
    plane_pos = jnp.arange(length, dtype=jnp.float32)[None, :]
    waves = ((row_index + 1) // 2).astype(jnp.float32)
    angles = 2.0 * math.pi * waves * plane_pos / length
    factor = math.sqrt(2.0 / length)
    result = jnp.where(row_index % 2 == 1, factor * jnp.cos(angles), factor * jnp.sin(angles))
    result = jnp.where(row_index == 0, 1.0 / math.sqrt(length), result)
    result = jnp.where(
        row_index == length - 1, jnp.cos(math.pi * plane_pos) / math.sqrt(length), result
    )
    return result


def node_masks():
    slots = np.arange(NB)[:, None]
    cells = jnp.arange(ELX * ELY)[None, :]
    row_ids = lax.axis_index("ex") * ELX + cells // ELY
    col_ids = lax.axis_index("ey") * ELY + cells % ELY
    rows_total = ELX * lax.axis_size("ex")
    cols_total = ELY * lax.axis_size("ey")
    on_left = jnp.asarray((slots == 0) | (slots >= 3 * P_SIZE))
    on_right = jnp.asarray((slots >= P_SIZE) & (slots <= 2 * P_SIZE))
    on_bottom = jnp.asarray(slots <= P_SIZE)
    on_top = jnp.asarray((slots >= 2 * P_SIZE) & (slots <= 3 * P_SIZE))
    dropped = (
        on_left & (row_ids == 0)
        | on_right & (row_ids == rows_total - 1)
        | on_bottom & (col_ids == 0)
        | on_top & (col_ids == cols_total - 1)
    )
    keep = jnp.where(dropped, 0.0, 1.0).astype(jnp.float32)
    corner_weight = jnp.asarray(np.where(slots % P_SIZE == 0, 0.25, 0.5).astype(np.float32))
    return keep, keep * corner_weight


def split_high_low(values):
    high = lax.reduce_precision(values, 8, 7)
    return high.astype(jnp.bfloat16), (values - high).astype(jnp.bfloat16)


def cg_kernel(
    modes,
    cond_ref,
    schur_ref,
    scale_ref,
    keep_ref,
    weight_ref,
    x_ref,
    res_ref,
    app_ref,
    dir_ref,
    along_ref,
    xs_ref,
    xr_ref,
    ys_ref,
    yr_ref,
    ps_ref,
    pr_ex,
    pr_ey,
    halo_send,
    halo_recv,
    sum_send_ex,
    sum_recv_ex,
    sum_send_ey,
    sum_recv_ey,
):
    cells = cond_ref.shape[1]
    sizes = {axis: lax.axis_size(axis) for axis in ("ex", "ey")}
    place = {axis: lax.axis_index(axis) for axis in ("ex", "ey")}
    lane = lax.broadcasted_iota(jnp.int32, (modes, cells), 1)
    lane_row = lane // ELY
    lane_col = lane % ELY

    def node(n):
        if isinstance(n, int):
            return pl.ds(n * modes, modes)
        return pl.ds(pl.multiple_of(n * modes, modes), modes)

    def turned(value, shift):
        shift = shift % cells
        return pltpu.roll(value, shift, 1) if shift else value

    xr_ref[...] = jnp.zeros_like(xr_ref)
    yr_ref[...] = jnp.zeros_like(yr_ref)

    barrier = pltpu.get_barrier_semaphore()
    for axis in ("ex", "ey"):
        for hop in range(1, sizes[axis]):
            pl.semaphore_signal(
                barrier,
                inc=1,
                device_id={axis: lax.rem(place[axis] + hop, sizes[axis])},
                device_id_type=pl.DeviceIdType.MESH,
            )
    for ex_step in (1, -1):
        for ey_step in (1, -1):
            pl.semaphore_signal(
                barrier,
                inc=1,
                device_id={
                    "ex": lax.rem(place["ex"] + ex_step + sizes["ex"], sizes["ex"]),
                    "ey": lax.rem(place["ey"] + ey_step + sizes["ey"], sizes["ey"]),
                },
                device_id_type=pl.DeviceIdType.MESH,
            )
    pl.semaphore_wait(barrier, sizes["ex"] + sizes["ey"] + 2)

    def exists(axis, step):
        if step == 0:
            return None
        return place[axis] < sizes[axis] - 1 if step > 0 else place[axis] > 0

    def guarded(ex_step, ey_step, action):
        tests = [t for t in (exists("ex", ex_step), exists("ey", ey_step)) if t is not None]
        pl.when(functools.reduce(jnp.logical_and, tests))(action)

    def halo_copy(turn, number, source, target, ex_step, ey_step):
        copy = pltpu.make_async_remote_copy(
            src_ref=source,
            dst_ref=target,
            send_sem=halo_send.at[turn, number],
            recv_sem=halo_recv.at[turn, number],
            device_id={
                "ex": lax.rem(place["ex"] + ex_step + sizes["ex"], sizes["ex"]),
                "ey": lax.rem(place["ey"] + ey_step + sizes["ey"], sizes["ey"]),
            },
            device_id_type=pl.DeviceIdType.MESH,
        )
        guarded(ex_step, ey_step, copy.start)

        def arrive():
            guarded(-ex_step, -ey_step, copy.wait_recv)

        def leave():
            guarded(ex_step, ey_step, copy.wait_send)

        return arrive, leave

    def assemble(ref, turn):
        bottom = lambda k: k
        top = lambda k: 3 * P_SIZE - k
        up = jnp.zeros((modes, cells), jnp.float32)
        down = up
        for k in range(P_SIZE + 1):
            up = jnp.where(lane_col == k, turned(ref[node(top(k)), :], k - ELY + 1), up)
            down = jnp.where(lane_col == k, turned(ref[node(bottom(k)), :], k), down)
        ys_ref[turn, 0] = up
        ys_ref[turn, 1] = down
        copies = []
        for slot, ex_step in ((1, 1), (2, -1), (0, 0)):
            for way, ey_step in ((0, 1), (1, -1)):
                copies.append(
                    halo_copy(
                        turn,
                        2 * slot + way,
                        ys_ref.at[turn, way],
                        yr_ref.at[turn, slot, way],
                        ex_step,
                        ey_step,
                    )
                )

        left = lambda k: (NB - k) % NB
        right = lambda k: P_SIZE + k
        last = cells - ELY
        up = jnp.zeros((modes, cells), jnp.float32)
        down = up
        for k in range(P_SIZE):
            up = jnp.where(lane_row == k, turned(ref[node(right(k)), :], ELY * k - last), up)
            down = jnp.where(lane_row == k, turned(ref[node(left(k)), :], ELY * k), down)
        xs_ref[turn, 0, 0] = up
        xs_ref[turn, 1, 0] = down
        xs_ref[turn, 0, 1] = turned(ref[node(right(P_SIZE)), :], -last)
        xs_ref[turn, 1, 1] = ref[node(left(P_SIZE)), :]
        for way, ex_step in ((0, 1), (1, -1)):
            copies.append(
                halo_copy(turn, 6 + way, xs_ref.at[turn, way], xr_ref.at[turn, way], ex_step, 0)
            )

        for k in range(P_SIZE + 1):
            here_left, here_right = ref[node(left(k)), :], ref[node(right(k)), :]
            ref[node(left(k)), :] = here_left + jnp.where(
                lane_row == 0, 0.0, turned(here_right, ELY)
            )
            ref[node(right(k)), :] = here_right + jnp.where(
                lane_row == ELX - 1, 0.0, turned(here_left, -ELY)
            )
        for arrive, _ in copies:
            arrive()

        for k in range(P_SIZE + 1):
            part, lanes = divmod(k, P_SIZE)
            low = turned(xr_ref[turn, 0, part], -ELY * lanes)
            high = turned(xr_ref[turn, 1, part], last - ELY * lanes)
            for n, halo, row in ((left(k), low, 0), (right(k), high, ELX - 1)):
                value = ref[node(n), :] + jnp.where(lane_row == row, halo, 0.0)
                if n % (2 * P_SIZE) > P_SIZE:
                    value = value * keep_ref[n : n + 1, :]
                ref[node(n), :] = value

        lines = []
        for way in range(2):
            line = yr_ref[turn, 0, way]
            before = jnp.where(
                lane == 0, turned(yr_ref[turn, 1, way], P_SIZE), turned(line, P_SIZE)
            )
            after = jnp.where(
                lane == last + P_SIZE, turned(yr_ref[turn, 2, way], -P_SIZE), turned(line, -P_SIZE)
            )
            lines.append(
                line
                + jnp.where(lane_col == 0, before, jnp.where(lane_col == P_SIZE, after, 0.0))
            )
        low_all, high_all = lines
        for k in range(P_SIZE + 1):
            b, t = bottom(k), top(k)
            here_bottom, here_top = ref[node(b), :], ref[node(t), :]
            ref[node(b), :] = keep_ref[b : b + 1, :] * (
                here_bottom
                + jnp.where(lane_col == 0, turned(low_all, -k), turned(here_top, 1))
            )
            ref[node(t), :] = keep_ref[t : t + 1, :] * (
                here_top
                + jnp.where(
                    lane_col == ELY - 1, turned(high_all, ELY - 1 - k), turned(here_bottom, -1)
                )
            )
        for _, leave in copies:
            leave()

    def operator(turn):
        scale = scale_ref[0:1, :]
        block = 8

        def step(outer, carry):
            for inner in range(block):
                mode = outer * block + inner
                value = res_ref[pl.ds(mode, NB, stride=modes), :]
                high = value.astype(jnp.bfloat16)
                low = (value - high.astype(jnp.float32)).astype(jnp.bfloat16)
                image = jnp.dot(
                    schur_ref[mode],
                    jnp.concatenate([high, low, high], 0),
                    preferred_element_type=jnp.float32,
                )
                app_ref[pl.ds(mode, NB, stride=modes), :] = image * scale
            return carry

        lax.fori_loop(0, modes // block, step, 0)
        assemble(app_ref, turn)

    def group_sum(mine, axis, turn, stage, slots, send_sem, recv_sem):
        ps_ref[turn, stage] = mine
        copies = [
            pltpu.make_async_remote_copy(
                src_ref=ps_ref.at[turn, stage],
                dst_ref=slots.at[turn, hop - 1],
                send_sem=send_sem.at[turn, hop - 1],
                recv_sem=recv_sem.at[turn, hop - 1],
                device_id={axis: lax.rem(place[axis] + hop, sizes[axis])},
                device_id_type=pl.DeviceIdType.MESH,
            )
            for hop in range(1, sizes[axis])
        ]
        for copy in copies:
            copy.start()
        for hop, copy in enumerate(copies):
            copy.wait_recv()
            mine = mine + slots[turn, hop]
        for copy in copies:
            copy.wait_send()
        return mine

    def paired(turn):
        def step(n, sums):
            weighted = weight_ref[pl.ds(n, 1), :] * res_ref[node(n), :]
            return (
                sums[0] + weighted * res_ref[node(n), :],
                sums[1] + weighted * app_ref[node(n), :],
            )

        zero = jnp.zeros((modes, cells), jnp.float32)
        norm, curve = lax.fori_loop(0, NB, step, (zero, zero))
        total = lax.dot_general(
            jnp.ones((8, cells), jnp.float32),
            jnp.concatenate([norm, curve], 0),
            (((1,), (1,)), ((), ())),
            precision=HIGHEST,
            preferred_element_type=jnp.float32,
        )
        total = group_sum(total, "ey", turn, 0, pr_ey, sum_send_ey, sum_recv_ey)
        total = group_sum(total, "ex", turn, 1, pr_ex, sum_send_ex, sum_recv_ex)
        row = lax.broadcasted_iota(jnp.int32, (modes, 2 * modes), 0)
        column = lax.broadcasted_iota(jnp.int32, (modes, 2 * modes), 1)
        pick = lambda offset: jnp.sum(
            jnp.where(column == row + offset, total[0:1, :], 0.0), axis=1, keepdims=True
        )
        return pick(0), pick(modes)

    res_ref[...] = cond_ref[...]
    assemble(res_ref, 0)
    for ref in (x_ref, dir_ref, along_ref):
        ref[...] = jnp.zeros_like(ref)

    def sweep(turn, scalars):
        norm_now, step_size = scalars
        operator(turn + 1)
        norm_next, curve_now = paired(turn)
        conj_ratio = jnp.where(turn == 0, 0.0, norm_next / norm_now)
        step_size = norm_next / (curve_now - conj_ratio * norm_next / step_size)

        def update(n, carry):
            rows = node(n)
            search = res_ref[rows, :] + conj_ratio * dir_ref[rows, :]
            along = app_ref[rows, :] + conj_ratio * along_ref[rows, :]
            x_ref[rows, :] = x_ref[rows, :] + step_size * search
            dir_ref[rows, :] = search
            along_ref[rows, :] = along
            res_ref[rows, :] = res_ref[rows, :] - step_size * along
            return carry

        lax.fori_loop(0, NB, update, 0)
        return norm_next, step_size

    one = jnp.ones((modes, 1), jnp.float32)
    lax.fori_loop(0, ITERS, sweep, (one, one))


def conjugate_gradients(condensed, stacked, scaling, keep, weights):
    modes, cells = condensed.shape[1:]
    field = pltpu.VMEM((NB * modes, cells), jnp.float32)
    along_ex, along_ey = lax.axis_size("ex") - 1, lax.axis_size("ey") - 1
    turns = ITERS + 1
    strips = lambda *lead: pltpu.VMEM(lead + (modes, cells), jnp.float32)
    tile = lambda *lead: pltpu.VMEM(lead + (8, 2 * modes), jnp.float32)
    semaphores = lambda *dims: pltpu.SemaphoreType.DMA(dims)
    whole = pl.BlockSpec(memory_space=pltpu.VMEM)
    solved = pl.pallas_call(
        functools.partial(cg_kernel, modes),
        out_shape=jax.ShapeDtypeStruct((NB * modes, cells), jnp.float32),
        in_specs=[whole] * 5,
        out_specs=whole,
        scratch_shapes=[field] * 4
        + [
            strips(turns, 2, 2),
            strips(turns, 2, 2),
            strips(turns, 2),
            strips(turns, 3, 2),
            tile(ITERS, 2),
            tile(ITERS, along_ex),
            tile(ITERS, along_ey),
            semaphores(turns, 8),
            semaphores(turns, 8),
            semaphores(ITERS, along_ex),
            semaphores(ITERS, along_ex),
            semaphores(ITERS, along_ey),
            semaphores(ITERS, along_ey),
        ],
        compiler_params=pltpu.CompilerParams(
            collective_id=0, has_side_effects=True, vmem_limit_bytes=40 << 20
        ),
        cost_estimate=pl.CostEstimate(flops=10**9, bytes_accessed=2 * 10**8, transcendentals=0),
    )(condensed.reshape(NB * modes, cells), stacked, scaling[None], keep, weights)
    return solved.reshape(NB, modes, cells)


def on_device(forcing, element_coef, schur, couple, inner_inv, element_cell):
    modes_dev = schur.shape[0]
    planes_dev = forcing.shape[0]
    elements = forcing.shape[2]
    groups = lax.axis_size("fourier")
    me = lax.axis_index("fourier")
    dft_table = dft_rows(modes_dev * groups)
    swap = [[(i, (i + hop) % groups) for i in range(groups)] for hop in range(groups)]
    plane_of = lambda group: lax.dynamic_slice_in_dim(dft_table, group * planes_dev, planes_dev, 1)
    rows_of = lambda table, group: lax.dynamic_slice_in_dim(table, group * modes_dev, modes_dev, 0)

    own_planes = plane_of(me)
    one_hot = (element_cell[:, None] == jnp.arange(elements)[None, :]).astype(jnp.float32)
    scaling = jnp.einsum("e,ec->c", element_coef, one_hot, precision=HIGHEST)

    order = [(me - hop) % groups for hop in range(groups)]
    middle = couple.shape[1] // 2
    folded = jnp.concatenate([couple[:, :middle], couple[:, middle:]], 0)
    couples = [couple]
    for hop in range(1, groups):
        arrived = lax.ppermute(folded, "fourier", swap[hop])
        couples.append(jnp.concatenate([arrived[:modes_dev], arrived[modes_dev:]], 1))

    partial = []
    condensed = None
    for hop in range(groups):
        spec = jnp.einsum(
            "mz,zne->mne", rows_of(own_planes, order[hop]), forcing, precision=HIGH
        )
        partial.append(spec[:, NB:])
        term = spec[:, :NB] - jnp.einsum("mbi,mie->mbe", couples[hop], spec[:, NB:], precision=HIGH)
        if hop:
            term = lax.ppermute(term, "fourier", [(b, a) for a, b in swap[hop]])
        condensed = term if condensed is None else condensed + term

    half, inner_count = modes_dev // 2, inner_inv.shape[2]
    padded = jnp.pad(inner_inv, ((0, 0), (0, 0), (0, elements // 2 - inner_count)))
    parcel = jnp.concatenate(
        [forcing[:, NB:], jnp.concatenate([padded[:half], padded[half:]], 2)], 0
    )
    keep, weights = node_masks()
    high, low = split_high_low(schur)
    stacked = jnp.concatenate([high, high, low], 2)
    condensed, parcel, stacked, scaling, keep, weights = lax.optimization_barrier(
        (condensed, parcel, stacked, scaling, keep, weights)
    )
    parcels = [None] + [lax.ppermute(parcel, "fourier", swap[h]) for h in range(1, groups)]
    condensed = jnp.einsum("mbe,ec->bmc", condensed, one_hot, precision=HIGH)
    iterate = conjugate_gradients(condensed, stacked, scaling, keep, weights)
    iterate = jnp.einsum("bmc,ec->mbe", iterate, one_hot, precision=HIGH)

    cycles = [iterate] + [lax.ppermute(iterate, "fourier", swap[h]) for h in range(1, groups)]
    bases = []
    for hop in range(groups):
        inverse = inner_inv
        if hop:
            pairs = parcels[hop][planes_dev:]
            inverse = jnp.concatenate(
                [pairs[:, :, :inner_count], pairs[:, :, elements // 2 :][:, :, :inner_count]], 0
            )
        inner = partial[hop]
        for far in range(1, groups):
            inner = inner + jnp.einsum(
                "mz,zne->mne",
                rows_of(plane_of(order[far]), order[hop]),
                parcels[far][:planes_dev],
                precision=HIGH,
            )
        bases.append(jnp.einsum("mij,mje->mie", inverse, inner, precision=HIGH) / element_coef)

    def back(hop, cycle, base):
        interior = base - jnp.einsum("mbi,mbe->mie", couples[hop], cycle, precision=HIGH)
        return jnp.einsum(
            "mz,mne->zne",
            rows_of(own_planes, order[hop]),
            jnp.concatenate([cycle, interior], 1),
            precision=HIGH,
        )

    velocity = back(0, iterate, bases[0])
    velocity, bases, cycles = lax.optimization_barrier((velocity, bases[1:], cycles[1:]))
    for hop in range(1, groups):
        velocity = velocity + back(hop, cycles[hop - 1], bases[hop - 1])
    return velocity


def solution(mesh):
    placed = (
        P("fourier", None, ("ex", "ey")),
        P(("ex", "ey")),
        P("fourier", None, None),
        P("fourier", None, None),
        P("fourier", None, None),
        P(("ex", "ey")),
    )
    return jax.shard_map(
        on_device,
        mesh=mesh,
        in_specs=placed,
        out_specs=P("fourier", None, ("ex", "ey")),
        check_vma=False,
    )
```

```python
import functools
import math

import jax
import jax.numpy as jnp
import numpy as np
from jax import lax
from jax.experimental import pallas as pl
from jax.experimental.pallas import tpu as pltpu
from jax.sharding import PartitionSpec as P

P_SIZE = 8
ITERS = 3
ELX = 8
ELY = 16
NB = 4 * P_SIZE
HIGH = lax.Precision.HIGH
HIGHEST = lax.Precision.HIGHEST


def dft_rows(length):
    row_index = jnp.arange(length)[:, None]
    plane_pos = jnp.arange(length, dtype=jnp.float32)[None, :]
    waves = ((row_index + 1) // 2).astype(jnp.float32)
    angles = 2.0 * math.pi * waves * plane_pos / length
    factor = math.sqrt(2.0 / length)
    result = jnp.where(row_index % 2 == 1, factor * jnp.cos(angles), factor * jnp.sin(angles))
    result = jnp.where(row_index == 0, 1.0 / math.sqrt(length), result)
    result = jnp.where(
        row_index == length - 1, jnp.cos(math.pi * plane_pos) / math.sqrt(length), result
    )
    return result


def node_masks():
    slots = np.arange(NB)[:, None]
    cells = jnp.arange(ELX * ELY)[None, :]
    row_ids = lax.axis_index("ex") * ELX + cells // ELY
    col_ids = lax.axis_index("ey") * ELY + cells % ELY
    rows_total = ELX * lax.axis_size("ex")
    cols_total = ELY * lax.axis_size("ey")
    on_left = jnp.asarray((slots == 0) | (slots >= 3 * P_SIZE))
    on_right = jnp.asarray((slots >= P_SIZE) & (slots <= 2 * P_SIZE))
    on_bottom = jnp.asarray(slots <= P_SIZE)
    on_top = jnp.asarray((slots >= 2 * P_SIZE) & (slots <= 3 * P_SIZE))
    dropped = (
        on_left & (row_ids == 0)
        | on_right & (row_ids == rows_total - 1)
        | on_bottom & (col_ids == 0)
        | on_top & (col_ids == cols_total - 1)
    )
    keep = jnp.where(dropped, 0.0, 1.0).astype(jnp.float32)
    corner_weight = jnp.asarray(np.where(slots % P_SIZE == 0, 0.25, 0.5).astype(np.float32))
    return keep, keep * corner_weight


def split_high_low(values):
    high = lax.reduce_precision(values, 8, 7)
    return high.astype(jnp.bfloat16), (values - high).astype(jnp.bfloat16)


def cg_kernel(
    modes,
    cond_ref,
    schur_ref,
    scale_ref,
    keep_ref,
    weight_ref,
    x_ref,
    res_ref,
    app_ref,
    dir_ref,
    along_ref,
    xs_ref,
    xr_ref,
    ys_ref,
    yr_ref,
    ps_ref,
    pr_ex,
    pr_ey,
    halo_send,
    halo_recv,
    sum_send_ex,
    sum_recv_ex,
    sum_send_ey,
    sum_recv_ey,
):
    cells = cond_ref.shape[1]
    sizes = {axis: lax.axis_size(axis) for axis in ("ex", "ey")}
    place = {axis: lax.axis_index(axis) for axis in ("ex", "ey")}
    lane = lax.broadcasted_iota(jnp.int32, (modes, cells), 1)
    lane_row = lane // ELY
    lane_col = lane % ELY

    def node(n):
        if isinstance(n, int):
            return pl.ds(n * modes, modes)
        return pl.ds(pl.multiple_of(n * modes, modes), modes)

    def turned(value, shift):
        shift = shift % cells
        return pltpu.roll(value, shift, 1) if shift else value

    xr_ref[...] = jnp.zeros_like(xr_ref)
    yr_ref[...] = jnp.zeros_like(yr_ref)

    barrier = pltpu.get_barrier_semaphore()
    for axis in ("ex", "ey"):
        for hop in range(1, sizes[axis]):
            pl.semaphore_signal(
                barrier,
                inc=1,
                device_id={axis: lax.rem(place[axis] + hop, sizes[axis])},
                device_id_type=pl.DeviceIdType.MESH,
            )
    for ex_step in (1, -1):
        for ey_step in (1, -1):
            pl.semaphore_signal(
                barrier,
                inc=1,
                device_id={
                    "ex": lax.rem(place["ex"] + ex_step + sizes["ex"], sizes["ex"]),
                    "ey": lax.rem(place["ey"] + ey_step + sizes["ey"], sizes["ey"]),
                },
                device_id_type=pl.DeviceIdType.MESH,
            )
    pl.semaphore_wait(barrier, sizes["ex"] + sizes["ey"] + 2)

    def exists(axis, step):
        if step == 0:
            return None
        return place[axis] < sizes[axis] - 1 if step > 0 else place[axis] > 0

    def guarded(ex_step, ey_step, action):
        tests = [t for t in (exists("ex", ex_step), exists("ey", ey_step)) if t is not None]
        pl.when(functools.reduce(jnp.logical_and, tests))(action)

    def halo_copy(turn, number, source, target, ex_step, ey_step):
        copy = pltpu.make_async_remote_copy(
            src_ref=source,
            dst_ref=target,
            send_sem=halo_send.at[turn, number],
            recv_sem=halo_recv.at[turn, number],
            device_id={
                "ex": lax.rem(place["ex"] + ex_step + sizes["ex"], sizes["ex"]),
                "ey": lax.rem(place["ey"] + ey_step + sizes["ey"], sizes["ey"]),
            },
            device_id_type=pl.DeviceIdType.MESH,
        )
        guarded(ex_step, ey_step, copy.start)

        def arrive():
            guarded(-ex_step, -ey_step, copy.wait_recv)

        def leave():
            guarded(ex_step, ey_step, copy.wait_send)

        return arrive, leave

    def assemble(ref, turn):
        bottom = lambda k: k
        top = lambda k: 3 * P_SIZE - k
        up = jnp.zeros((modes, cells), jnp.float32)
        down = up
        for k in range(P_SIZE + 1):
            up = jnp.where(lane_col == k, turned(ref[node(top(k)), :], k - ELY + 1), up)
            down = jnp.where(lane_col == k, turned(ref[node(bottom(k)), :], k), down)
        ys_ref[turn, 0] = up
        ys_ref[turn, 1] = down
        copies = []
        for slot, ex_step in ((1, 1), (2, -1), (0, 0)):
            for way, ey_step in ((0, 1), (1, -1)):
                copies.append(
                    halo_copy(
                        turn,
                        2 * slot + way,
                        ys_ref.at[turn, way],
                        yr_ref.at[turn, slot, way],
                        ex_step,
                        ey_step,
                    )
                )

        left = lambda k: (NB - k) % NB
        right = lambda k: P_SIZE + k
        last = cells - ELY
        up = jnp.zeros((modes, cells), jnp.float32)
        down = up
        for k in range(P_SIZE):
            up = jnp.where(lane_row == k, turned(ref[node(right(k)), :], ELY * k - last), up)
            down = jnp.where(lane_row == k, turned(ref[node(left(k)), :], ELY * k), down)
        xs_ref[turn, 0, 0] = up
        xs_ref[turn, 1, 0] = down
        xs_ref[turn, 0, 1] = turned(ref[node(right(P_SIZE)), :], -last)
        xs_ref[turn, 1, 1] = ref[node(left(P_SIZE)), :]
        for way, ex_step in ((0, 1), (1, -1)):
            copies.append(
                halo_copy(turn, 6 + way, xs_ref.at[turn, way], xr_ref.at[turn, way], ex_step, 0)
            )

        for k in range(P_SIZE + 1):
            here_left, here_right = ref[node(left(k)), :], ref[node(right(k)), :]
            ref[node(left(k)), :] = here_left + jnp.where(
                lane_row == 0, 0.0, turned(here_right, ELY)
            )
            ref[node(right(k)), :] = here_right + jnp.where(
                lane_row == ELX - 1, 0.0, turned(here_left, -ELY)
            )
        for arrive, _ in copies:
            arrive()

        for k in range(P_SIZE + 1):
            part, lanes = divmod(k, P_SIZE)
            low = turned(xr_ref[turn, 0, part], -ELY * lanes)
            high = turned(xr_ref[turn, 1, part], last - ELY * lanes)
            for n, halo, row in ((left(k), low, 0), (right(k), high, ELX - 1)):
                value = ref[node(n), :] + jnp.where(lane_row == row, halo, 0.0)
                if n % (2 * P_SIZE) > P_SIZE:
                    value = value * keep_ref[n : n + 1, :]
                ref[node(n), :] = value

        lines = []
        for way in range(2):
            line = yr_ref[turn, 0, way]
            before = jnp.where(
                lane == 0, turned(yr_ref[turn, 1, way], P_SIZE), turned(line, P_SIZE)
            )
            after = jnp.where(
                lane == last + P_SIZE, turned(yr_ref[turn, 2, way], -P_SIZE), turned(line, -P_SIZE)
            )
            lines.append(
                line
                + jnp.where(lane_col == 0, before, jnp.where(lane_col == P_SIZE, after, 0.0))
            )
        low_all, high_all = lines
        for k in range(P_SIZE + 1):
            b, t = bottom(k), top(k)
            here_bottom, here_top = ref[node(b), :], ref[node(t), :]
            ref[node(b), :] = keep_ref[b : b + 1, :] * (
                here_bottom
                + jnp.where(lane_col == 0, turned(low_all, -k), turned(here_top, 1))
            )
            ref[node(t), :] = keep_ref[t : t + 1, :] * (
                here_top
                + jnp.where(
                    lane_col == ELY - 1, turned(high_all, ELY - 1 - k), turned(here_bottom, -1)
                )
            )
        for _, leave in copies:
            leave()

    def operator(turn):
        scale = scale_ref[0:1, :]
        block = 8

        def step(outer, carry):
            for inner in range(block):
                mode = outer * block + inner
                value = res_ref[pl.ds(mode, NB, stride=modes), :]
                high = value.astype(jnp.bfloat16)
                low = (value - high.astype(jnp.float32)).astype(jnp.bfloat16)
                image = jnp.dot(
                    schur_ref[mode],
                    jnp.concatenate([high, low, high], 0),
                    preferred_element_type=jnp.float32,
                )
                app_ref[pl.ds(mode, NB, stride=modes), :] = image * scale
            return carry

        lax.fori_loop(0, modes // block, step, 0)
        assemble(app_ref, turn)

    def group_sum(mine, axis, turn, stage, slots, send_sem, recv_sem):
        ps_ref[turn, stage] = mine
        copies = [
            pltpu.make_async_remote_copy(
                src_ref=ps_ref.at[turn, stage],
                dst_ref=slots.at[turn, hop - 1],
                send_sem=send_sem.at[turn, hop - 1],
                recv_sem=recv_sem.at[turn, hop - 1],
                device_id={axis: lax.rem(place[axis] + hop, sizes[axis])},
                device_id_type=pl.DeviceIdType.MESH,
            )
            for hop in range(1, sizes[axis])
        ]
        for copy in copies:
            copy.start()
        for hop, copy in enumerate(copies):
            copy.wait_recv()
            mine = mine + slots[turn, hop]
        for copy in copies:
            copy.wait_send()
        return mine

    def paired(turn):
        def step(n, sums):
            weighted = weight_ref[pl.ds(n, 1), :] * res_ref[node(n), :]
            return (
                sums[0] + weighted * res_ref[node(n), :],
                sums[1] + weighted * app_ref[node(n), :],
            )

        zero = jnp.zeros((modes, cells), jnp.float32)
        norm, curve = lax.fori_loop(0, NB, step, (zero, zero))
        total = lax.dot_general(
            jnp.ones((8, cells), jnp.float32),
            jnp.concatenate([norm, curve], 0),
            (((1,), (1,)), ((), ())),
            precision=HIGHEST,
            preferred_element_type=jnp.float32,
        )
        total = group_sum(total, "ey", turn, 0, pr_ey, sum_send_ey, sum_recv_ey)
        total = group_sum(total, "ex", turn, 1, pr_ex, sum_send_ex, sum_recv_ex)
        row = lax.broadcasted_iota(jnp.int32, (modes, 2 * modes), 0)
        column = lax.broadcasted_iota(jnp.int32, (modes, 2 * modes), 1)
        pick = lambda offset: jnp.sum(
            jnp.where(column == row + offset, total[0:1, :], 0.0), axis=1, keepdims=True
        )
        return pick(0), pick(modes)

    res_ref[...] = cond_ref[...]
    assemble(res_ref, 0)
    for ref in (x_ref, dir_ref, along_ref):
        ref[...] = jnp.zeros_like(ref)

    def sweep(turn, scalars):
        norm_now, step_size = scalars
        operator(turn + 1)
        norm_next, curve_now = paired(turn)
        conj_ratio = jnp.where(turn == 0, 0.0, norm_next / norm_now)
        step_size = norm_next / (curve_now - conj_ratio * norm_next / step_size)

        def update(n, carry):
            rows = node(n)
            search = res_ref[rows, :] + conj_ratio * dir_ref[rows, :]
            along = app_ref[rows, :] + conj_ratio * along_ref[rows, :]
            x_ref[rows, :] = x_ref[rows, :] + step_size * search
            dir_ref[rows, :] = search
            along_ref[rows, :] = along
            res_ref[rows, :] = res_ref[rows, :] - step_size * along
            return carry

        lax.fori_loop(0, NB, update, 0)
        return norm_next, step_size

    one = jnp.ones((modes, 1), jnp.float32)
    lax.fori_loop(0, ITERS, sweep, (one, one))


def conjugate_gradients(condensed, stacked, scaling, keep, weights):
    modes, cells = condensed.shape[1:]
    field = pltpu.VMEM((NB * modes, cells), jnp.float32)
    along_ex, along_ey = lax.axis_size("ex") - 1, lax.axis_size("ey") - 1
    turns = ITERS + 1
    strips = lambda *lead: pltpu.VMEM(lead + (modes, cells), jnp.float32)
    tile = lambda *lead: pltpu.VMEM(lead + (8, 2 * modes), jnp.float32)
    semaphores = lambda *dims: pltpu.SemaphoreType.DMA(dims)
    whole = pl.BlockSpec(memory_space=pltpu.VMEM)
    solved = pl.pallas_call(
        functools.partial(cg_kernel, modes),
        out_shape=jax.ShapeDtypeStruct((NB * modes, cells), jnp.float32),
        in_specs=[whole] * 5,
        out_specs=whole,
        scratch_shapes=[field] * 4
        + [
            strips(turns, 2, 2),
            strips(turns, 2, 2),
            strips(turns, 2),
            strips(turns, 3, 2),
            tile(ITERS, 2),
            tile(ITERS, along_ex),
            tile(ITERS, along_ey),
            semaphores(turns, 8),
            semaphores(turns, 8),
            semaphores(ITERS, along_ex),
            semaphores(ITERS, along_ex),
            semaphores(ITERS, along_ey),
            semaphores(ITERS, along_ey),
        ],
        compiler_params=pltpu.CompilerParams(
            collective_id=0, has_side_effects=True, vmem_limit_bytes=40 << 20
        ),
        cost_estimate=pl.CostEstimate(flops=10**9, bytes_accessed=2 * 10**8, transcendentals=0),
    )(condensed.reshape(NB * modes, cells), stacked, scaling[None], keep, weights)
    return solved.reshape(NB, modes, cells)


def on_device(forcing, element_coef, schur, couple, inner_inv, element_cell):
    modes_dev = schur.shape[0]
    planes_dev = forcing.shape[0]
    elements = forcing.shape[2]
    groups = lax.axis_size("fourier")
    me = lax.axis_index("fourier")
    dft_table = dft_rows(modes_dev * groups)
    swap = [[(i, (i + hop) % groups) for i in range(groups)] for hop in range(groups)]
    plane_of = lambda group: lax.dynamic_slice_in_dim(dft_table, group * planes_dev, planes_dev, 1)
    rows_of = lambda table, group: lax.dynamic_slice_in_dim(table, group * modes_dev, modes_dev, 0)

    own_planes = plane_of(me)
    one_hot = (element_cell[:, None] == jnp.arange(elements)[None, :]).astype(jnp.float32)
    scaling = jnp.einsum("e,ec->c", element_coef, one_hot, precision=HIGHEST)

    order = [(me - hop) % groups for hop in range(groups)]
    middle = couple.shape[1] // 2
    folded = jnp.concatenate([couple[:, :middle], couple[:, middle:]], 0)
    couples = [couple]
    for hop in range(1, groups):
        arrived = lax.ppermute(folded, "fourier", swap[hop])
        couples.append(jnp.concatenate([arrived[:modes_dev], arrived[modes_dev:]], 1))

    partial = []
    condensed = None
    for hop in range(groups):
        spec = jnp.einsum(
            "mz,zne->mne", rows_of(own_planes, order[hop]), forcing, precision=HIGH
        )
        partial.append(spec[:, NB:])
        term = spec[:, :NB] - jnp.einsum("mbi,mie->mbe", couples[hop], spec[:, NB:], precision=HIGH)
        if hop:
            term = lax.ppermute(term, "fourier", [(b, a) for a, b in swap[hop]])
        condensed = term if condensed is None else condensed + term

    half, inner_count = modes_dev // 2, inner_inv.shape[2]
    padded = jnp.pad(inner_inv, ((0, 0), (0, 0), (0, elements // 2 - inner_count)))
    parcel = jnp.concatenate(
        [forcing[:, NB:], jnp.concatenate([padded[:half], padded[half:]], 2)], 0
    )
    keep, weights = node_masks()
    high, low = split_high_low(schur)
    stacked = jnp.concatenate([high, high, low], 2)
    condensed, parcel, stacked, scaling, keep, weights = lax.optimization_barrier(
        (condensed, parcel, stacked, scaling, keep, weights)
    )
    parcels = [None] + [lax.ppermute(parcel, "fourier", swap[h]) for h in range(1, groups)]
    condensed = jnp.einsum("mbe,ec->bmc", condensed, one_hot, precision=HIGH)
    iterate = conjugate_gradients(condensed, stacked, scaling, keep, weights)
    iterate = jnp.einsum("bmc,ec->mbe", iterate, one_hot, precision=HIGH)
    iterate, inner_inv = lax.optimization_barrier((iterate, inner_inv))

    cycles = [iterate] + [lax.ppermute(iterate, "fourier", swap[h]) for h in range(1, groups)]
    bases = []
    for hop in range(groups):
        inverse = inner_inv
        if hop:
            pairs = parcels[hop][planes_dev:]
            inverse = jnp.concatenate(
                [pairs[:, :, :inner_count], pairs[:, :, elements // 2 :][:, :, :inner_count]], 0
            )
        inner = partial[hop]
        for far in range(1, groups):
            inner = inner + jnp.einsum(
                "mz,zne->mne",
                rows_of(plane_of(order[far]), order[hop]),
                parcels[far][:planes_dev],
                precision=HIGH,
            )
        bases.append(jnp.einsum("mij,mje->mie", inverse, inner, precision=HIGH) / element_coef)

    def back(hop, cycle, base):
        interior = base - jnp.einsum("mbi,mbe->mie", couples[hop], cycle, precision=HIGH)
        return jnp.einsum(
            "mz,mne->zne",
            rows_of(own_planes, order[hop]),
            jnp.concatenate([cycle, interior], 1),
            precision=HIGH,
        )

    velocity = back(0, iterate, bases[0])
    velocity, bases, cycles = lax.optimization_barrier((velocity, bases[1:], cycles[1:]))
    for hop in range(1, groups):
        velocity = velocity + back(hop, cycles[hop - 1], bases[hop - 1])
    return velocity


def solution(mesh):
    placed = (
        P("fourier", None, ("ex", "ey")),
        P(("ex", "ey")),
        P("fourier", None, None),
        P("fourier", None, None),
        P("fourier", None, None),
        P(("ex", "ey")),
    )
    return jax.shard_map(
        on_device,
        mesh=mesh,
        in_specs=placed,
        out_specs=P("fourier", None, ("ex", "ey")),
        check_vma=False,
    )
```
